32 devices in a mesh: groups: 2 (over x), space: 16 (over z, y, core).
Axes of the slice: x: 2, y: 2, z: 4, core: 2. Of those that a mesh axis runs over, the one named last changes fastest.
Arguments:
- inputs: bfloat16 [768, 1152, 256], P(('groups', 'space')), parts along dimension 0, may hold values from -6 to 6
- spectral_weight: bfloat16 [2, 256, 2, 256, 256], P(None, 'space'), may hold values from -0.25 to 0.25
- local_weight: bfloat16 [2, 256, 256], replicated, may hold values from -0.375 to 0.375
- layer_bias: bfloat16 [2, 256], replicated, may hold values from -3 to 3
- readout_hidden: bfloat16 [256, 256], replicated, may hold values from -0.375 to 0.375
- readout_final: bfloat16 [20, 256], replicated, may hold values from -0.375 to 0.375
Outputs:
- forecast: bfloat16 [20, 768, 1152], P(None, ('groups', 'space')), parts along dimension 1
The draws below stay inside these ranges and needn't reach their ends.
There are 2 independent parts, one for each index of `groups`. The reference program is written for one: setup_inputs(seed, part) draws one part's arguments, and reference() takes and returns one part's arrays. A program takes and returns all parts, laid end to end along the dimension named above; an argument that names none is the same for every part. Nothing has to cross between parts.
All inputs are finite; a program needn't handle non-finite values.
Results may differ from the reference program's by a relative error of at most 0.018.
Values may be sent and summed in bfloat16 or wider, within the bound.
A program may use at most 128 MiB of HBM per device.

```python
import jax
import jax.numpy as jnp
from jax import lax

H = 384
W = 1152
C = 256
KY = 16
KX = 16
LAYERS = 2
QH = 256
VARS = 20
MODES = 256
N_SPACE = 16


def block_scale(rng, extent, cuts, smallest, top_value):
    gain, own = 1.0, jax.random.fold_in(rng, 6)
    for axis_at, blocks in cuts:
        heights = jnp.exp(jax.random.uniform(jax.random.fold_in(own, axis_at), (blocks,), jnp.float32, smallest / len(cuts), top_value / len(cuts)))
        gain = gain * jnp.repeat(heights, extent[axis_at] // blocks).reshape([-1 if axis == axis_at else 1 for axis in range(len(extent))])
    return gain


def gaussian(rng, extent, scale, reach, cuts=(), kind=jnp.bfloat16):
    drawn = jax.random.normal(rng, extent, jnp.float32) * scale
    if len(cuts) > 0:
        drawn = block_scale(rng, extent, cuts, -0.22, 0.18) * drawn
    return jnp.clip(drawn, min=-reach, max=reach).astype(kind)


def setup_inputs(seed: int = 0, part: int = 0) -> dict:
    key_list = jax.random.split(jax.random.key(seed), 7)
    own_keys = jax.random.split(jax.random.fold_in(key_list[6], part), 7)
    return {
        "inputs": gaussian(own_keys[0], (H, W, C), 1.0, 6.0, ((0, 16),)),
        "spectral_weight": gaussian(key_list[1], (LAYERS, MODES, 2, C, C), (2 * C) ** -0.5, 0.25, ((1, 16),)),
        "local_weight": gaussian(key_list[2], (LAYERS, C, C), C ** -0.5, 0.375),
        "layer_bias": gaussian(key_list[3], (LAYERS, C), 0.5, 3.0),
        "readout_hidden": gaussian(key_list[4], (C, QH), C ** -0.5, 0.375),
        "readout_final": gaussian(key_list[5], (VARS, QH), QH ** -0.5, 0.375),
    }


def zonal_tables(columns, modes):
    column_ids = jnp.arange(columns, dtype=jnp.int32)
    wave_numbers = jnp.arange(1, modes + 1, dtype=jnp.int32)
    phase_int = column_ids[:, None] * wave_numbers[None, :] % columns
    angles = 2.0 * jnp.pi / columns * phase_int.astype(jnp.float32)
    cosines = jnp.cos(angles)
    sines = jnp.sin(angles)
    forward = jnp.concatenate([cosines, -sines], axis=1) / jnp.sqrt(jnp.float32(columns))
    inverse = jnp.stack([cosines, -sines], axis=2).reshape(columns, 2 * modes) * jnp.sqrt(jnp.float32(2.0 / modes))
    return (forward.astype(jnp.bfloat16), inverse.astype(jnp.bfloat16))

def meridional_tables(row_ids, height, modes):
    mode_index = jnp.arange(modes, dtype=jnp.int32)
    wave_numbers = jnp.where(mode_index < modes // 2, mode_index, mode_index - modes)
    phase_int = wave_numbers[:, None] * row_ids[None, :] % height
    angles = 2.0 * jnp.pi / height * phase_int.astype(jnp.float32)
    cosines = jnp.cos(angles)
    sines = jnp.sin(angles)
    forward = jnp.stack([jnp.stack([cosines, sines], axis=2), jnp.stack([-sines, cosines], axis=2)], axis=1)
    forward = forward / jnp.sqrt(jnp.float32(height))
    cos_rows = cosines.T
    sin_rows = sines.T
    inverse = jnp.stack([jnp.stack([cos_rows, -sin_rows], axis=2), jnp.stack([sin_rows, cos_rows], axis=2)], axis=1)
    inverse = inverse / jnp.sqrt(jnp.float32(modes))
    return (forward.astype(jnp.bfloat16), inverse.astype(jnp.bfloat16))

def mix_modes(spectrum, weights):
    real_in = spectrum[:, 0].astype(jnp.float32)
    imag_in = spectrum[:, 1].astype(jnp.float32)
    real_weight = weights[:, 0].astype(jnp.float32)
    imag_weight = weights[:, 1].astype(jnp.float32)

    def product(vectors, matrices):
        return jnp.einsum('mi,mio->mo', vectors, matrices)
    real_out = product(real_in, real_weight) - product(imag_in, imag_weight)
    imag_out = product(real_in, imag_weight) + product(imag_in, real_weight)
    return jnp.stack([real_out, imag_out], axis=1).astype(jnp.bfloat16)

def reference(inputs, spectral_weight, local_weight, layer_bias, readout_hidden, readout_final):
    height, columns, channels = inputs.shape
    blocks = height // 64
    zonal_forward, zonal_inverse = zonal_tables(columns, KX)
    rows_each = height // N_SPACE
    stored_rows = jnp.arange(height, dtype=jnp.int32)
    row_ids = (stored_rows % rows_each * N_SPACE + stored_rows // rows_each).astype(jnp.int32)
    meridional_forward, meridional_inverse = meridional_tables(row_ids, height, KY)
    current = inputs
    for layer_index in range(LAYERS):

        def zonal_block(block_rows):
            return jnp.einsum('hwc,wj->hjc', block_rows.astype(jnp.float32), zonal_forward.astype(jnp.float32)).astype(jnp.bfloat16)
        zonal_part = lax.map(zonal_block, current.reshape(blocks, 64, columns, channels))
        zonal_view = zonal_part.reshape(height, 2, KX, channels)
        spectrum = jnp.einsum('qphr,hrkc->qkpc', meridional_forward.astype(jnp.float32), zonal_view.astype(jnp.float32))
        spectrum = spectrum.reshape(MODES, 2, channels).astype(jnp.bfloat16)
        mixed = mix_modes(spectrum, spectral_weight[layer_index]).reshape(KY, KX, 2, channels)
        returned = jnp.einsum('hpqr,qkrc->hkpc', meridional_inverse.astype(jnp.float32), mixed.astype(jnp.float32))
        returned = returned.astype(jnp.bfloat16).reshape(blocks, 64, 2 * KX, channels)
        weight_now = local_weight[layer_index]
        bias_now = layer_bias[layer_index].astype(jnp.float32)

        def finish(block_pair):
            block_rows, block_back = block_pair
            spread = jnp.einsum('wj,hjc->hwc', zonal_inverse.astype(jnp.float32), block_back.astype(jnp.float32))
            pointwise = jnp.dot(block_rows.reshape(-1, channels), weight_now, preferred_element_type=jnp.float32)
            pointwise = pointwise.reshape(block_rows.shape)
            return jax.nn.gelu(spread + pointwise + bias_now, approximate=True).astype(jnp.bfloat16)
        current = lax.map(finish, (current.reshape(blocks, 64, columns, channels), returned))
        current = current.reshape(height, columns, channels)

    def readout(block_rows):
        flat_rows = block_rows.reshape(-1, channels)
        hidden = jax.nn.gelu(jnp.dot(flat_rows, readout_hidden, preferred_element_type=jnp.float32), approximate=True)
        hidden = hidden.astype(jnp.bfloat16)
        final = jnp.einsum('pq,nq->pn', readout_final.astype(jnp.float32), hidden.astype(jnp.float32))
        return final.astype(jnp.bfloat16).reshape(readout_final.shape[0], 64, columns)
    pieces = lax.map(readout, current.reshape(blocks, 64, columns, channels))
    return jnp.transpose(pieces, (1, 0, 2, 3)).reshape(readout_final.shape[0], height, columns)
```

```python
import functools

import jax
import jax.numpy as jnp
import numpy as np
from jax import lax
from jax.experimental import pallas as pl
from jax.experimental.pallas import tpu as pltpu
from jax.sharding import PartitionSpec as P

KY = 16
KX = 16
LAYERS = 2
MODES = KY * KX
BF16 = jnp.bfloat16
F32 = jnp.float32
VMEM_LIMIT = 60 * 1024 * 1024


def zonal_tables(columns):
    phase = np.arange(columns)[:, None] * np.arange(1, KX + 1)[None, :] % columns
    angles = np.float32(2.0 * np.pi / columns) * phase.astype(np.float32)
    cosines, sines = np.cos(angles), np.sin(angles)
    forward = np.concatenate([cosines, -sines], axis=1) / np.sqrt(np.float32(columns))
    inverse = np.stack([cosines, -sines], axis=2).reshape(columns, 2 * KX)
    inverse = inverse * np.sqrt(np.float32(2.0 / KX))
    extended = np.zeros((columns, 128), np.float32)
    extended[:, : 2 * KX] = inverse
    extended[:, 2 * KX] = 1.0
    return forward.T.astype(BF16), extended.astype(BF16)


def meridional_tables(rows_here, devices):
    height = rows_here * devices
    rows = np.arange(rows_here)[None, :] * devices + np.arange(devices)[:, None]
    index = np.arange(KY)
    waves = np.where(index < KY // 2, index, index - KY)
    phase = waves[None, :, None] * rows[:, None, :] % height
    angles = np.float32(2.0 * np.pi / height) * phase.astype(np.float32)
    cosines, sines = np.cos(angles), np.sin(angles)
    forward = np.stack(
        [np.stack([cosines, sines], -1), np.stack([-sines, cosines], -1)], axis=2
    ) / np.sqrt(np.float32(height))
    cos_rows, sin_rows = cosines.transpose(0, 2, 1), sines.transpose(0, 2, 1)
    inverse = np.stack(
        [np.stack([cos_rows, -sin_rows], -1), np.stack([sin_rows, cos_rows], -1)], axis=2
    ) / np.sqrt(np.float32(KY))
    return (
        forward.reshape(devices, 2 * KY, 2 * rows_here).astype(BF16),
        inverse.reshape(devices, 2 * rows_here, 2 * KY).astype(BF16),
    )


def one_hot(values, count):
    return (values[:, None] == np.arange(count)[None, :]).astype(BF16)


def expanded_tables(rows_here, devices, me):
    forward, inverse = meridional_tables(rows_here, devices)
    owned = MODES // devices
    spectral = np.arange(2 * MODES)
    mode = spectral // (2 * owned) * owned + spectral % owned
    part = spectral // owned % 2
    spectral_wave = mode % KX
    spectral_qp = mode // KX * 2 + part
    rows = np.arange(rows_here * 2 * KX)
    zonal_hr, zonal_wave = rows // KX, rows % KX
    back_hp, back_wave = rows // (2 * KX) * 2 + rows % 2, rows % (2 * KX) // 2
    here = lax.dynamic_index_in_dim(jnp.asarray(forward), me, keepdims=False)
    back = lax.dynamic_index_in_dim(jnp.asarray(inverse), me, keepdims=False)
    pick_qp = jnp.asarray(one_hot(spectral_qp, 2 * KY))

    def spread_out(left, middle, right, left_wave, right_wave):
        inner = jnp.dot(left, middle, preferred_element_type=F32).astype(BF16)
        full = jnp.dot(inner, right, preferred_element_type=F32)
        same = jnp.asarray(left_wave, jnp.int32)[:, None] == jnp.asarray(right_wave, jnp.int32)[None, :]
        return jnp.where(same, full, 0.0).astype(BF16)

    ahead = spread_out(
        pick_qp, here, jnp.asarray(one_hot(zonal_hr, 2 * rows_here).T), spectral_wave, zonal_wave
    )
    behind = spread_out(
        jnp.asarray(one_hot(back_hp, 2 * rows_here)), back, pick_qp.T, back_wave, spectral_wave
    )
    return ahead, behind


def gelu(v):
    inner = v * (0.7978845608028654 + (0.7978845608028654 * 0.044715) * (v * v))
    half = 0.5 * v
    return half + half * jnp.tanh(inner)


def analyse_row(zonal_ref, held_ref, state, row):
    part = jnp.dot(zonal_ref[...], state, preferred_element_type=F32)
    depth = zonal_ref.shape[0]
    held_ref[pl.ds(pl.multiple_of(row * depth, depth), depth), :] = part.astype(BF16)


def analyse_end(ahead_ref, held_ref, partial_ref):
    @pl.when(pl.program_id(0) == pl.num_programs(0) - 1)
    def _():
        sums = jnp.dot(ahead_ref[...], held_ref[...], preferred_element_type=F32)
        partial_ref[...] = sums.reshape(partial_ref.shape).astype(partial_ref.dtype)


def first_kernel(state_ref, zonal_ref, ahead_ref, partial_ref, held_ref):
    rows = state_ref.shape[0]
    for r in range(rows):
        analyse_row(zonal_ref, held_ref, state_ref[r], pl.program_id(0) * rows + r)
    analyse_end(ahead_ref, held_ref, partial_ref)


def update(state_ref, r, start, size, spread_ref, weight_ref, back_ref, bias_ref):
    left = jnp.concatenate(
        [state_ref[r, pl.ds(start, size), :], spread_ref[pl.ds(start, size), :]], axis=1
    )
    depth = 2 * KX
    back = back_ref[pl.ds(r * depth, depth), :]
    right = jnp.concatenate([weight_ref[...], back, bias_ref[...]], axis=0)
    return gelu(jnp.dot(left, right, preferred_element_type=F32)).astype(BF16)


def middle_kernel(
    chunk, state_ref, back_ref, spread_ref, weight_ref, bias_ref, zonal_ref, ahead_ref,
    next_ref, partial_ref, held_ref,
):
    rows, columns = state_ref.shape[:2]
    for r in range(rows):
        for start in range(0, columns, chunk):
            next_ref[r, pl.ds(start, chunk), :] = update(
                state_ref, r, start, chunk, spread_ref, weight_ref, back_ref, bias_ref
            )
        analyse_row(zonal_ref, held_ref, next_ref[r], pl.program_id(0) * rows + r)
    analyse_end(ahead_ref, held_ref, partial_ref)


def last_kernel(
    chunk, rows_here, state_ref, back_ref, spread_ref, weight_ref, bias_ref, hidden_ref, final_ref,
    out_ref, held_ref,
):
    rows, columns = state_ref.shape[:2]
    count = final_ref.shape[0]
    for r in range(rows):
        row = pl.program_id(0) * rows + r
        for start in range(0, columns, chunk):
            state = update(
                state_ref, r, start, chunk, spread_ref, weight_ref, back_ref, bias_ref
            )
            hidden = gelu(
                jnp.dot(state, hidden_ref[...], preferred_element_type=F32)
            ).astype(BF16)
            final = lax.dot_general(
                final_ref[...], hidden, (((1,), (1,)), ((), ())), preferred_element_type=F32
            )
            for lane in range(0, chunk, 128):
                held_ref[
                    (start + lane) // 128, pl.ds(row, count, stride=rows_here), :
                ] = final[:, lane : lane + 128]

    @pl.when(pl.program_id(0) == pl.num_programs(0) - 1)
    def _():
        for block in range(columns // 128):
            out_ref[:, pl.ds(block * 128, 128)] = held_ref[block].astype(BF16)


def exchange_kernel(
    layer, n, partial_ref, weight_hbm, behind_ref, back_ref,
    weights, arrived, mixed_ref, gathered, weight_sem, sent, received, sent_mixed, received_mixed,
):
    me = lax.axis_index("space")
    load = pltpu.make_async_copy(weight_hbm.at[layer], weights, weight_sem)
    load.start()
    barrier = pltpu.get_barrier_semaphore()
    for i in range(1, n):
        pl.semaphore_signal(barrier, inc=1, device_id={"space": lax.rem(me + i, n)})
    pl.semaphore_wait(barrier, n - 1)

    def part_copy(i):
        to = lax.rem(me + i, n)
        return pltpu.make_async_remote_copy(
            src_ref=partial_ref.at[to], dst_ref=arrived.at[i], send_sem=sent.at[i],
            recv_sem=received.at[i], device_id={"space": to},
        )

    def mixed_copy(i):
        return pltpu.make_async_remote_copy(
            src_ref=mixed_ref, dst_ref=gathered.at[me], send_sem=sent_mixed.at[i],
            recv_sem=received_mixed.at[i], device_id={"space": lax.rem(me + i, n)},
        )

    for i in range(1, n):
        part_copy(i).start()
    total = partial_ref[me].astype(F32)
    for i in range(1, n):
        part_copy(i).wait_recv()
        total = total + arrived[i].astype(F32)
    spectrum = total.astype(BF16)
    load.wait()
    owned = total.shape[0] // 2
    row = lax.broadcasted_iota(jnp.int32, (owned, total.shape[1]), 0)
    real = jnp.zeros((owned, total.shape[1]), F32)
    imag = jnp.zeros((owned, total.shape[1]), F32)
    for m in range(owned):
        by_real = jnp.dot(spectrum, weights[m, 0], preferred_element_type=F32)
        by_imag = jnp.dot(spectrum, weights[m, 1], preferred_element_type=F32)
        real = jnp.where(row == m, by_real[:owned] - by_imag[owned:], real)
        imag = jnp.where(row == m, by_imag[:owned] + by_real[owned:], imag)
    mixed = jnp.concatenate([real, imag], axis=0).astype(BF16)
    mixed_ref[...] = mixed
    for i in range(1, n):
        mixed_copy(i).start()
    gathered[me] = mixed
    for i in range(1, n):
        mixed_copy(i).wait_recv()
    modes = gathered[...].astype(F32).reshape(n * 2 * owned, -1).astype(BF16)
    back_ref[...] = jnp.dot(behind_ref[...], modes, preferred_element_type=F32).astype(BF16)
    for i in range(1, n):
        part_copy(i).wait_send()
        mixed_copy(i).wait_send()


def whole(shape):
    return pl.BlockSpec(shape, lambda i: (0,) * len(shape))


def params():
    return pltpu.CompilerParams(
        dimension_semantics=("arbitrary",), vmem_limit_bytes=VMEM_LIMIT
    )


def pick_chunk(columns):
    for chunk in (384, 256, 128):
        if columns % chunk == 0:
            return chunk
    return columns


def per_device(inputs, spectral_weight, local_weight, layer_bias, readout_hidden, readout_final):
    rows_here, columns, channels = inputs.shape
    n = lax.axis_size("space")
    owned = MODES // n
    depth = 2 * KX
    step = 2 if rows_here % 2 == 0 else 1
    steps = rows_here // step
    chunk = pick_chunk(columns)
    count = readout_final.shape[0]
    zonal_np, spread_np = zonal_tables(columns)
    zonal, spread = jnp.asarray(zonal_np), jnp.asarray(spread_np)
    ahead, behind = expanded_tables(rows_here, n, lax.axis_index("space"))
    bias_rows = jnp.pad(layer_bias[:, None, :], ((0, 0), (0, 127 - depth), (0, 0)))

    state_spec = pl.BlockSpec((step, columns, channels), lambda i: (i, 0, 0))
    back_spec = pl.BlockSpec((step * depth, channels), lambda i: (i, 0))
    partial_shape = (n, 2 * owned, channels)
    partial_out = jax.ShapeDtypeStruct(partial_shape, BF16)
    held = pltpu.VMEM((rows_here * depth, channels), BF16)

    def exchange(layer, partial):
        vmem = pl.BlockSpec(memory_space=pltpu.VMEM)
        return pl.pallas_call(
            functools.partial(exchange_kernel, layer, n),
            name=f"exchange_{layer}",
            out_shape=jax.ShapeDtypeStruct((rows_here * depth, channels), BF16),
            in_specs=[vmem, pl.BlockSpec(memory_space=pl.ANY), vmem],
            out_specs=vmem,
            scratch_shapes=[
                pltpu.VMEM((owned, 2, channels, channels), BF16),
                pltpu.VMEM(partial_shape, BF16),
                pltpu.VMEM((2 * owned, channels), BF16),
                pltpu.VMEM(partial_shape, BF16),
                pltpu.SemaphoreType.DMA,
                pltpu.SemaphoreType.DMA((n,)),
                pltpu.SemaphoreType.DMA((n,)),
                pltpu.SemaphoreType.DMA((n,)),
                pltpu.SemaphoreType.DMA((n,)),
            ],
            compiler_params=pltpu.CompilerParams(
                collective_id=layer, has_side_effects=True, vmem_limit_bytes=VMEM_LIMIT
            ),
        )(partial, spectral_weight, behind)

    partial = pl.pallas_call(
        first_kernel,
        name="first",
        grid=(steps,),
        out_shape=partial_out,
        in_specs=[state_spec, whole(zonal.shape), whole(ahead.shape)],
        out_specs=whole(partial_shape),
        scratch_shapes=[held],
        compiler_params=params(),
    )(inputs, zonal, ahead)
    current = inputs
    for layer in range(LAYERS - 1):
        back = exchange(layer, partial)
        current, partial = pl.pallas_call(
            functools.partial(middle_kernel, chunk),
            name=f"middle_{layer}",
            grid=(steps,),
            out_shape=(jax.ShapeDtypeStruct(inputs.shape, BF16), partial_out),
            in_specs=[
                state_spec, back_spec, whole(spread.shape), whole((channels, channels)),
                whole(bias_rows.shape[1:]), whole(zonal.shape), whole(ahead.shape),
            ],
            out_specs=(state_spec, whole(partial_shape)),
            scratch_shapes=[held],
            compiler_params=params(),
        )(current, back, spread, local_weight[layer], bias_rows[layer], zonal, ahead)
    layer = LAYERS - 1
    back = exchange(layer, partial)
    forecast = pl.pallas_call(
        functools.partial(last_kernel, chunk, rows_here),
        name="last",
        grid=(steps,),
        out_shape=jax.ShapeDtypeStruct((count * rows_here, columns), BF16),
        in_specs=[
            state_spec, back_spec, whole(spread.shape), whole((channels, channels)),
            whole(bias_rows.shape[1:]), whole(readout_hidden.shape), whole(readout_final.shape),
        ],
        out_specs=whole((count * rows_here, columns)),
        scratch_shapes=[pltpu.VMEM((columns // 128, count * rows_here, 128), F32)],
        compiler_params=params(),
    )(current, back, spread, local_weight[layer], bias_rows[layer], readout_hidden, readout_final)
    return forecast.reshape(count, rows_here, columns)


def solution(mesh):
    in_specs = (
        P(("groups", "space"), None, None),
        P(None, "space", None, None, None),
        P(),
        P(),
        P(),
        P(),
    )
    out_specs = P(None, ("groups", "space"), None)
    return jax.shard_map(
        per_device, mesh=mesh, in_specs=in_specs, out_specs=out_specs, check_vma=False
    )
```

```python
import functools

import jax
import jax.numpy as jnp
import numpy as np
from jax import lax
from jax.experimental import pallas as pl
from jax.experimental.pallas import tpu as pltpu
from jax.sharding import PartitionSpec as P

KY = 16
KX = 16
LAYERS = 2
MODES = KY * KX
BF16 = jnp.bfloat16
F32 = jnp.float32
VMEM_LIMIT = 62 * 1024 * 1024
GELU_TYPE = BF16
SLOPE = 0.7978845608028654


def zonal_tables(columns):
    phase = np.arange(columns)[:, None] * np.arange(1, KX + 1)[None, :] % columns
    angles = np.float32(2.0 * np.pi / columns) * phase.astype(np.float32)
    cosines, sines = np.cos(angles), np.sin(angles)
    forward = np.concatenate([cosines, -sines], axis=1) / np.sqrt(np.float32(columns))
    inverse = np.stack([cosines, -sines], axis=2).reshape(columns, 2 * KX)
    inverse = inverse * np.sqrt(np.float32(2.0 / KX))
    extended = np.zeros((columns, 128), np.float32)
    extended[:, : 2 * KX] = inverse
    extended[:, 2 * KX] = 1.0
    return forward.T.astype(BF16), extended.astype(BF16)


def meridional_tables(rows_here, devices):
    height = rows_here * devices
    rows = np.arange(rows_here)[None, :] * devices + np.arange(devices)[:, None]
    index = np.arange(KY)
    waves = np.where(index < KY // 2, index, index - KY)
    phase = waves[None, :, None] * rows[:, None, :] % height
    angles = np.float32(2.0 * np.pi / height) * phase.astype(np.float32)
    cosines, sines = np.cos(angles), np.sin(angles)
    forward = np.stack(
        [np.stack([cosines, sines], -1), np.stack([-sines, cosines], -1)], axis=2
    ) / np.sqrt(np.float32(height))
    cos_rows, sin_rows = cosines.transpose(0, 2, 1), sines.transpose(0, 2, 1)
    inverse = np.stack(
        [np.stack([cos_rows, -sin_rows], -1), np.stack([sin_rows, cos_rows], -1)], axis=2
    ) / np.sqrt(np.float32(KY))
    return (
        forward.reshape(devices, 2 * KY, 2 * rows_here).astype(BF16),
        inverse.reshape(devices, 2 * rows_here, 2 * KY).astype(BF16),
    )


def shift_of(value):
    shift = value.bit_length() - 1
    assert 1 << shift == value
    return shift


def expand_tables(owned, forward, inverse, ahead_ref, behind_ref):
    wave_bits, owned_bits = shift_of(KX), shift_of(owned)

    def split(shape, axis):
        index = lax.broadcasted_iota(jnp.int32, shape, axis)
        part = (index >> owned_bits) & 1
        mode = ((index >> (owned_bits + 1)) << owned_bits) + (index & (owned - 1))
        return mode & (KX - 1), (mode >> wave_bits) * 2 + part

    def iota(shape, axis):
        return lax.broadcasted_iota(jnp.int32, shape, axis)

    def ones(mask):
        return jnp.where(mask, 1.0, 0.0).astype(BF16)

    def product(left, middle, right, same):
        inner = jnp.dot(left, middle, preferred_element_type=F32).astype(BF16)
        full = jnp.dot(inner, right, preferred_element_type=F32)
        return jnp.where(same, full, 0.0).astype(BF16)

    modes, wide = ahead_ref.shape
    narrow = forward.shape[1]
    qp = forward.shape[0]
    pick = ones(split((modes, qp), 0)[1] == iota((modes, qp), 1))
    rows = ones(iota((narrow, wide), 0) == iota((narrow, wide), 1) >> wave_bits)
    same = split((modes, wide), 0)[0] == iota((modes, wide), 1) & (KX - 1)
    ahead_ref[...] = product(pick, forward, rows, same)
    index = iota((wide, narrow), 0)
    rows = ones((index >> (wave_bits + 1)) * 2 + (index & 1) == iota((wide, narrow), 1))
    pick = ones(split((qp, modes), 1)[1] == iota((qp, modes), 0))
    same = (iota((wide, modes), 0) & (2 * KX - 1)) >> 1 == split((wide, modes), 1)[0]
    behind_ref[...] = product(rows, inverse, pick, same)


def gelu_of_half(half):
    half = half.astype(GELU_TYPE)
    inner = half * (SLOPE * 2.0 + (SLOPE * 0.044715 * 8.0) * (half * half))
    return (half + half * jnp.tanh(inner)).astype(BF16)


def program_kernel(
    n, chunk, state_hbm, weight_hbm, local_ref, bias_ref, hidden_ref, final_ref,
    zonal_ref, spread_ref, forward_ref, inverse_ref, out_ref,
    state_a, state_b, weights, ahead, behind, right, hidden_half, held, back,
    partial, arrived, mixed_ref, gathered, finals,
    state_sem, weight_sem, sent, received, sent_mixed, received_mixed,
):
    me = lax.axis_index("space")
    rows_here, columns, channels = state_a.shape
    owned = weights.shape[1]
    depth = 2 * KX
    count = final_ref.shape[0]
    load_rows = 2 if rows_here % 2 == 0 else 1
    work_rows = next(k for k in (4, 3, 2, 1) if rows_here % k == 0)
    last_rows = load_rows

    def state_copy(j):
        rows = pl.ds(j * load_rows, load_rows)
        return pltpu.make_async_copy(state_hbm.at[rows], state_a.at[rows], state_sem.at[j])

    def weight_copy(layer):
        return pltpu.make_async_copy(
            weight_hbm.at[layer], weights.at[layer], weight_sem.at[layer]
        )

    def part_copy(layer, i):
        to = lax.rem(me + i, n)
        return pltpu.make_async_remote_copy(
            src_ref=partial.at[layer, to], dst_ref=arrived.at[layer, i],
            send_sem=sent.at[layer, i], recv_sem=received.at[layer, i],
            device_id={"space": to},
        )

    def mixed_copy(layer, i):
        return pltpu.make_async_remote_copy(
            src_ref=mixed_ref.at[layer], dst_ref=gathered.at[layer, me],
            send_sem=sent_mixed.at[layer, i], recv_sem=received_mixed.at[layer, i],
            device_id={"space": lax.rem(me + i, n)},
        )

    for j in range(rows_here // load_rows):
        state_copy(j).start()
    for layer in range(LAYERS):
        weight_copy(layer).start()
    barrier = pltpu.get_barrier_semaphore()
    for i in range(1, n):
        pl.semaphore_signal(barrier, inc=1, device_id={"space": lax.rem(me + i, n)})
    expand_tables(owned, forward_ref[me], inverse_ref[me], ahead, behind)
    hidden_half[...] = (0.5 * hidden_ref[...].astype(F32)).astype(BF16)

    def analyse(state, row):
        part = jnp.dot(zonal_ref[...], state[row], preferred_element_type=F32)
        held[pl.ds(pl.multiple_of(row * depth, depth), depth), :] = part.astype(BF16)

    def exchange(layer):
        sums = jnp.dot(ahead[...], held[...], preferred_element_type=F32)
        partial[layer] = sums.reshape(n, 2 * owned, channels).astype(BF16)
        if layer == 0:
            pl.semaphore_wait(barrier, n - 1)
        for i in range(1, n):
            part_copy(layer, i).start()
        total = partial[layer, me].astype(F32)
        first = lax.broadcasted_iota(jnp.int32, (128 - depth, channels), 0) == 0
        bias = bias_ref[layer : layer + 1, :].astype(F32)
        right[:channels, :] = (0.5 * local_ref[layer].astype(F32)).astype(BF16)
        right[channels:, :] = jnp.where(first, 0.5 * bias, 0.0).astype(BF16)
        weight_copy(layer).wait()
        for i in range(1, n):
            part_copy(layer, i).wait_recv()
            total = total + arrived[layer, i].astype(F32)
        spectrum = total.astype(BF16)
        row = lax.broadcasted_iota(jnp.int32, (owned, channels), 0)
        real = jnp.zeros((owned, channels), F32)
        imag = jnp.zeros((owned, channels), F32)
        for m in range(owned):
            by_real = jnp.dot(spectrum, weights[layer, m, 0], preferred_element_type=F32)
            by_imag = jnp.dot(spectrum, weights[layer, m, 1], preferred_element_type=F32)
            real = jnp.where(row == m, by_real[:owned] - by_imag[owned:], real)
            imag = jnp.where(row == m, by_imag[:owned] + by_real[owned:], imag)
        mixed = jnp.concatenate([real, imag], axis=0).astype(BF16)
        mixed_ref[layer] = mixed
        for i in range(1, n):
            mixed_copy(layer, i).start()
        gathered[layer, me] = mixed
        for i in range(1, n):
            mixed_copy(layer, i).wait_recv()
        modes = gathered[layer].astype(F32).reshape(n * 2 * owned, channels).astype(BF16)
        values = jnp.dot(behind[...], modes, preferred_element_type=F32).astype(BF16)
        back[...] = (0.5 * values.astype(F32)).astype(BF16)
        for i in range(1, n):
            part_copy(layer, i).wait_send()
            mixed_copy(layer, i).wait_send()

    def update(state, row, start):
        columns_now = pl.ds(start, chunk)
        left = jnp.concatenate([state[row, columns_now, :], spread_ref[columns_now, :]], axis=1)
        returned = back[pl.ds(pl.multiple_of(row * depth, depth), depth), :]
        table = jnp.concatenate([right[:channels, :], returned, right[channels:, :]], axis=0)
        return gelu_of_half(jnp.dot(left, table, preferred_element_type=F32))

    def first_step(j, carry):
        state_copy(j).wait()
        for r in range(load_rows):
            analyse(state_a, j * load_rows + r)
        return carry

    lax.fori_loop(0, rows_here // load_rows, first_step, 0)
    source, target = state_a, state_b
    for layer in range(LAYERS - 1):
        exchange(layer)

        def middle_step(j, carry, source=source, target=target):
            for r in range(work_rows):
                row = j * work_rows + r
                for start in range(0, columns, chunk):
                    target[row, pl.ds(start, chunk), :] = update(source, row, start)
                analyse(target, row)
            return carry

        lax.fori_loop(0, rows_here // work_rows, middle_step, 0)
        source, target = target, source
    exchange(LAYERS - 1)

    def last_step(j, carry):
        for r in range(last_rows):
            row = j * last_rows + r
            for start in range(0, columns, chunk):
                state = update(source, row, start)
                hidden = gelu_of_half(
                    jnp.dot(state, hidden_half[...], preferred_element_type=F32)
                )
                final = lax.dot_general(
                    final_ref[...], hidden, (((1,), (1,)), ((), ())), preferred_element_type=F32
                )
                for lane in range(0, chunk, 128):
                    finals[
                        (start + lane) // 128, pl.ds(row, count, stride=rows_here), :
                    ] = final[:, lane : lane + 128]
        return carry

    lax.fori_loop(0, rows_here // last_rows, last_step, 0)
    for block in range(columns // 128):
        out_ref[:, pl.ds(block * 128, 128)] = finals[block].astype(BF16)


def pick_chunk(columns):
    return next((chunk for chunk in (384, 256, 128) if columns % chunk == 0), columns)


def per_device(inputs, spectral_weight, local_weight, layer_bias, readout_hidden, readout_final):
    rows_here, columns, channels = inputs.shape
    n = lax.axis_size("space")
    owned = MODES // n
    depth = 2 * KX
    count = readout_final.shape[0]
    zonal, spread = zonal_tables(columns)
    forward, inverse = meridional_tables(rows_here, n)
    vmem = pl.BlockSpec(memory_space=pltpu.VMEM)
    anywhere = pl.BlockSpec(memory_space=pl.ANY)
    chunks = (LAYERS, n, 2 * owned, channels)
    dma = pltpu.SemaphoreType.DMA
    forecast = pl.pallas_call(
        functools.partial(program_kernel, n, pick_chunk(columns)),
        name="program",
        out_shape=jax.ShapeDtypeStruct((count * rows_here, columns), BF16),
        in_specs=[anywhere, anywhere] + [vmem] * 8,
        out_specs=vmem,
        scratch_shapes=[
            pltpu.VMEM(inputs.shape, BF16),
            pltpu.VMEM(inputs.shape, BF16),
            pltpu.VMEM((LAYERS, owned, 2, channels, channels), BF16),
            pltpu.VMEM((2 * MODES, rows_here * depth), BF16),
            pltpu.VMEM((rows_here * depth, 2 * MODES), BF16),
            pltpu.VMEM((channels + 128 - depth, channels), BF16),
            pltpu.VMEM(readout_hidden.shape, BF16),
            pltpu.VMEM((rows_here * depth, channels), BF16),
            pltpu.VMEM((rows_here * depth, channels), BF16),
            pltpu.VMEM(chunks, BF16),
            pltpu.VMEM(chunks, BF16),
            pltpu.VMEM((LAYERS, 2 * owned, channels), BF16),
            pltpu.VMEM(chunks, BF16),
            pltpu.VMEM((columns // 128, count * rows_here, 128), F32),
            dma((rows_here,)),
            dma((LAYERS,)),
            dma((LAYERS, n)),
            dma((LAYERS, n)),
            dma((LAYERS, n)),
            dma((LAYERS, n)),
        ],
        compiler_params=pltpu.CompilerParams(
            collective_id=0, has_side_effects=True, vmem_limit_bytes=VMEM_LIMIT
        ),
    )(
        inputs, spectral_weight, local_weight, layer_bias, readout_hidden, readout_final,
        jnp.asarray(zonal), jnp.asarray(spread), jnp.asarray(forward), jnp.asarray(inverse),
    )
    return forecast.reshape(count, rows_here, columns)


def solution(mesh):
    in_specs = (
        P(("groups", "space"), None, None),
        P(None, "space", None, None, None),
        P(),
        P(),
        P(),
        P(),
    )
    out_specs = P(None, ("groups", "space"), None)
    return jax.shard_map(
        per_device, mesh=mesh, in_specs=in_specs, out_specs=out_specs, check_vma=False
    )
```
